32 devices in a mesh: col: 16 (over z, y, x), sec: 2 (over core).
Axes of the slice: x: 2, y: 2, z: 4, core: 2. Of those that a mesh axis runs over, the one named last changes fastest.
Arguments:
- mps: bfloat16 [16, 96, 6, 6, 96], P('col', 'sec'), may hold values from -6 to 6
- ket: bfloat16 [16, 6, 6, 6, 6, 2], P('col'), may hold values from -6 to 6
- left_proj: bfloat16 [16, 96, 96, 6, 6], P('col', 'sec'), may hold values from -0.109375 to 0.109375
- right_proj: bfloat16 [16, 96, 6, 6, 96], P('col', None, None, None, 'sec'), may hold values from -0.109375 to 0.109375
- bond_charge: int32 [16, 96], P('col'), may hold values from 0 to 5
- new_charge: int32 [16, 96], P('col'), may hold values from 0 to 5
- link_charge: int32 [16, 6], P('col'), may hold values from 0 to 2
- vert_charge: int32 [16, 2, 6], P('col'), may hold values from 0 to 2
Outputs:
- new_mps: bfloat16 [16, 96, 6, 6, 96], P('col', 'sec')
- log_norm: float32 [], replicated
The draws below stay inside these ranges and needn't reach their ends.
All inputs are finite; a program needn't handle non-finite values.
Results may differ from the reference program's by a relative error of at most 0.0064.
Values may be sent and summed in bfloat16 or wider, within the bound.
A program may use at most 192 MiB of HBM per device.

```python
import jax
import jax.numpy as jnp
from jax import lax

CHI = 96
D = 6
P_SIZE = 2
SITES = 16


def with_ends(values, key, least, top_value):
    dims = values.shape
    index_at = [jax.random.randint(jax.random.fold_in(key, axis), (), 0, dims[axis]) for axis in range(len(dims))]
    values = values.at[tuple(index_at)].set(least)
    longest = dims.index(max(dims))
    index_at[longest] = (index_at[longest] + 1) % dims[longest]
    return values.at[tuple(index_at)].set(top_value)


def steps_of(rng, extent, split, low, largest):
    loudness = 1.0
    for dim, blocks in split:
        draws = jax.random.uniform(jax.random.fold_in(jax.random.fold_in(rng, 6), dim), (blocks,), jnp.float32, low / len(split), largest / len(split))
        loudness = loudness * jnp.repeat(jnp.exp(draws), extent[dim] // blocks).reshape((-1,) + (1,) * (len(extent) - 1 - dim))
    return loudness


def normal_values(stream_key, extent, deviation, most, cuts=(), held_as=jnp.bfloat16):
    entries = jax.random.normal(stream_key, extent, jnp.float32) * deviation
    if len(cuts) > 0:
        entries = steps_of(stream_key, extent, cuts, -0.22, 0.18) * entries
    return jnp.clip(entries, min=-most, max=most).astype(held_as)


def setup_inputs(seed: int = 0) -> dict:
    key_of = jax.random.split(jax.random.key(seed), 9)
    return {
        "mps": normal_values(key_of[0], (SITES, CHI, D, D, CHI), 1.0, 6.0, ((0, 16), (1, 2))),
        "ket": normal_values(key_of[1], (SITES, D, D, D, D, P_SIZE), 1.0, 6.0, ((0, 16),)),
        "left_proj": normal_values(key_of[2], (SITES, CHI, CHI, D, D), (CHI * D * D) ** -0.5, 0.109375, ((0, 16), (1, 2))),
        "right_proj": normal_values(key_of[3], (SITES, CHI, D, D, CHI), (CHI * D * D) ** -0.5, 0.109375, ((0, 16), (4, 2))),
        "bond_charge": with_ends(jax.random.randint(key_of[4], (SITES, CHI), 0, 6), jax.random.fold_in(key_of[4], 1), 0, 5).astype(jnp.int32),
        "new_charge": with_ends(jax.random.randint(key_of[5], (SITES, CHI), 0, 6), jax.random.fold_in(key_of[5], 1), 0, 5).astype(jnp.int32),
        "link_charge": with_ends(jax.random.randint(key_of[6], (SITES, D), 0, 3), jax.random.fold_in(key_of[6], 1), 0, 2).astype(jnp.int32),
        "vert_charge": with_ends(jax.random.randint(key_of[7], (SITES, 2, D), 0, 3), jax.random.fold_in(key_of[7], 1), 0, 2).astype(jnp.int32),
    }


def absorb(mps_site, ket_site, left_site, right_site, charge_here, charge_next, fresh_here, fresh_next, link_here, link_next, vertical):
    upper = vertical[0]
    lower = vertical[1]
    physical = jnp.arange(ket_site.shape[4], dtype=jnp.int32)
    keep_mps = charge_here[:, None, None, None] + upper[None, :, None, None] - upper[None, None, :, None] == charge_next[None, None, None, :]
    masked_mps = jnp.where(keep_mps, mps_site, jnp.zeros_like(mps_site))
    keep_ket = upper[:, None, None, None, None] + link_here[None, :, None, None, None] == lower[None, None, :, None, None] + link_next[None, None, None, :, None] + physical[None, None, None, None, :]
    masked_ket = jnp.where(keep_ket, ket_site, jnp.zeros_like(ket_site))
    keep_left = fresh_here[:, None, None, None] == charge_here[None, :, None, None] + link_here[None, None, :, None] - link_here[None, None, None, :]
    masked_left = jnp.where(keep_left, left_site, jnp.zeros_like(left_site))
    keep_right = charge_next[:, None, None, None] + link_next[None, :, None, None] - link_next[None, None, :, None] == fresh_next[None, None, None, :]
    masked_right = jnp.where(keep_right, right_site, jnp.zeros_like(right_site))
    ket_wide = masked_ket.astype(jnp.float32)
    first = jnp.einsum('xalm,auvb->xlmuvb', masked_left.astype(jnp.float32), masked_mps.astype(jnp.float32)).astype(jnp.bfloat16)
    second = jnp.einsum('xlmuvb,uldrp->xmvbdrp', first.astype(jnp.float32), ket_wide).astype(jnp.bfloat16)
    third = jnp.einsum('xmvbdrp,vmesp->xbdres', second.astype(jnp.float32), ket_wide).astype(jnp.bfloat16)
    return jnp.einsum('xbdres,brsy->xdey', third.astype(jnp.float32), masked_right.astype(jnp.float32))

def reference(mps, ket, left_proj, right_proj, bond_charge, new_charge, link_charge, vert_charge):

    def following(array):
        return jnp.roll(array, -1, axis=0)
    items = (mps, ket, left_proj, following(right_proj), bond_charge, following(bond_charge), new_charge, following(new_charge), link_charge, following(link_charge), vert_charge)

    def single(item):
        return absorb(*item)
    image = lax.map(single, items)
    count = CHI * D * D * CHI
    meansq = lax.optimization_barrier(jnp.sum(image * image, axis=(1, 2, 3, 4))) / count
    scale = lax.rsqrt(meansq + 1e-06)
    new_mps = (image * scale[:, None, None, None, None]).astype(jnp.bfloat16)
    log_norm = jnp.mean(0.5 * jnp.log(meansq + 1e-06))
    return (new_mps, log_norm)
```

```python
import functools

import jax
import jax.numpy as jnp
from jax import lax
from jax.experimental import pallas as pl
from jax.experimental.pallas import tpu as pltpu
from jax.sharding import PartitionSpec as P

LANES = 128
PACK = 8
F32 = jnp.float32
BF16 = jnp.bfloat16


def from_behind(x, axis, by):
    count = lax.axis_size(axis)
    return lax.ppermute(x, axis, [(i, (i + by) % count) for i in range(count)])


def chain(legs, block, left_ref, mps_ref, up_ref, down_ref, right_ref, out_ref, sq_ref, mps_s, w1, w2, w3):
    pairs = legs // 2
    rows = legs * PACK
    wide = block * LANES

    @pl.when(pl.program_id(0) == 0)
    def _():
        for uv in range(legs * legs):
            mps_s[:, uv * LANES : (uv + 1) * LANES] = mps_ref[uv]
        sq_ref[...] = jnp.zeros_like(sq_ref)

    for u in range(legs):
        for vp in range(pairs):
            at = (u * legs + 2 * vp) * LANES
            part = jnp.dot(left_ref[...], mps_s[:, at : at + 2 * LANES], preferred_element_type=F32).astype(BF16)
            for x in range(block):
                for mp in range(pairs):
                    lo = x * rows + mp * 2 * PACK
                    for v2 in range(2):
                        w1[vp, mp, v2 * legs + u, :, x * LANES : (x + 1) * LANES] = part[
                            lo : lo + 2 * PACK, v2 * LANES : (v2 + 1) * LANES
                        ]

    slab = w2.shape[2]

    def second(i, _):
        rhs = w1[i // pairs, i % pairs].reshape(2 * legs * 2 * PACK, wide)
        part = jnp.dot(up_ref[...], rhs, preferred_element_type=F32).astype(BF16)
        w2[:, i] = part.reshape(pairs * legs, slab, wide)
        return 0

    lax.fori_loop(0, pairs * pairs, second, 0)

    for dp in range(pairs):
        for r in range(legs):
            rhs = w2[dp * legs + r].reshape(pairs * pairs * slab, wide)
            part = jnp.dot(down_ref[...], rhs, preferred_element_type=F32).astype(BF16)
            for x in range(block):
                for s in range(legs):
                    lane = (r * legs + s) * LANES
                    row = x * rows + dp * 2 * PACK
                    w3[row : row + 2 * PACK, lane : lane + LANES] = part[
                        s * 2 * PACK : (s + 1) * 2 * PACK, x * LANES : (x + 1) * LANES
                    ]

    image = jnp.dot(w3[...], right_ref[...], preferred_element_type=F32)
    out_ref[...] = image
    sq_ref[...] += jnp.sum((image * image).reshape(block * rows // 8, 8, image.shape[1]), axis=0)


def local(mps, ket, left_proj, right_proj, bond_charge, new_charge, link_charge, vert_charge):
    half = left_proj.shape[1]
    full_mps = lax.all_gather(mps, "sec", axis=1, tiled=True)[0]
    chi = full_mps.shape[0]
    legs = full_mps.shape[1]
    phys = ket.shape[5]
    pairs = legs // 2
    rows = legs * PACK
    charges = jnp.concatenate([bond_charge, new_charge, link_charge], axis=1)
    got = from_behind(charges, "col", -1)[0]
    arrived = from_behind(right_proj, "col", -1)
    right = lax.all_gather(arrived, "sec", axis=4, tiled=True)[0]
    q_here = bond_charge[0]
    q_next = got[:chi]
    n_next = got[chi : 2 * chi]
    h_next = got[2 * chi :]
    h_here = link_charge[0]
    n_half = lax.dynamic_slice_in_dim(new_charge[0], lax.axis_index("sec") * half, half, 0)
    upper, lower = vert_charge[0, 0], vert_charge[0, 1]

    keep = (
        q_here[None, None, :, None] + upper[:, None, None, None] - upper[None, :, None, None]
        == q_next[None, None, None, :]
    )
    ms = jnp.where(keep, full_mps.transpose(1, 2, 0, 3), 0).reshape(legs * legs, chi, chi)
    ms = jnp.pad(ms, ((0, 0), (0, 0), (0, LANES - chi)))
    keep = (
        n_half[:, None, None, None]
        == q_here[None, None, None, :] + h_here[None, None, :, None] - h_here[None, :, None, None]
    )
    lp = jnp.where(keep, left_proj[0].transpose(0, 3, 2, 1), 0)
    lp = jnp.pad(lp, ((0, 0), (0, 0), (0, PACK - legs), (0, 0))).reshape(half * rows, chi)
    keep = (
        q_next[None, None, :, None] + h_next[:, None, None, None] - h_next[None, :, None, None]
        == n_next[None, None, None, :]
    )
    rp = jnp.where(keep, right.transpose(1, 2, 0, 3), 0)
    rp = jnp.pad(rp, ((0, 0), (0, 0), (0, LANES - chi), (0, 0))).reshape(legs * legs * LANES, chi)
    physical = jnp.arange(phys, dtype=jnp.int32)
    keep = (
        upper[:, None, None, None, None] + h_here[None, :, None, None, None]
        == lower[None, None, :, None, None] + h_next[None, None, None, :, None] + physical
    )
    ks = jnp.where(keep, ket[0], 0)
    ks8 = jnp.pad(ks, ((0, 0), (0, PACK - legs), (0, 0), (0, 0), (0, 0)))
    two = jnp.eye(2, dtype=BF16)
    up = jnp.einsum(
        "uldcrp,vw,mn->drcvmpwunl", ks8.reshape(legs, PACK, pairs, 2, legs, phys), two, two
    ).reshape(pairs * legs * 8 * phys, 2 * legs * 2 * PACK)
    kd = jnp.pad(ks, ((0, 0), (0, 0), (0, PACK - legs), (0, 0), (0, 0)))
    down = jnp.einsum("vwmnesp,dc->sdevmcwnp", kd.reshape(pairs, 2, pairs, 2, PACK, legs, phys), two).reshape(
        legs * 2 * PACK, pairs * pairs * 8 * phys
    )

    block = 8
    wide = block * LANES
    whole = lambda a: pl.BlockSpec(a.shape, lambda i: (0,) * a.ndim)
    image, squares = pl.pallas_call(
        functools.partial(chain, legs, block),
        grid=(half // block,),
        in_specs=[
            pl.BlockSpec((block * rows, chi), lambda i: (i, 0)),
            whole(ms),
            whole(up),
            whole(down),
            whole(rp),
        ],
        out_specs=[
            pl.BlockSpec((block * rows, chi), lambda i: (i, 0)),
            pl.BlockSpec((8, chi), lambda i: (0, 0)),
        ],
        out_shape=[
            jax.ShapeDtypeStruct((half * rows, chi), F32),
            jax.ShapeDtypeStruct((8, chi), F32),
        ],
        scratch_shapes=[
            pltpu.VMEM((chi, legs * legs * LANES), BF16),
            pltpu.VMEM((pairs, pairs, 2 * legs, 2 * PACK, wide), BF16),
            pltpu.VMEM((pairs * legs, pairs * pairs, 8 * phys, wide), BF16),
            pltpu.VMEM((block * rows, legs * legs * LANES), BF16),
        ],
        compiler_params=pltpu.CompilerParams(
            dimension_semantics=("arbitrary",), vmem_limit_bytes=56 * 1024 * 1024
        ),
    )(lp, ms, up, down, rp)

    sums = lax.all_gather(jnp.sum(squares).reshape(1), ("col", "sec"), axis=0, tiled=True)
    columns = lax.axis_size("col")
    meansq = jnp.sum(sums.reshape(columns, -1), axis=1) / (chi * legs * legs * chi)
    log_norm = jnp.mean(0.5 * jnp.log(meansq + 1e-06))
    mine = lax.dynamic_slice_in_dim(meansq, lax.axis_index("col"), 1, 0)[0]
    scale = lax.rsqrt(mine + 1e-06)
    image = image.reshape(half, legs, PACK, chi)[:, :, :legs, :]
    new_mps = (image * scale).astype(BF16)[None]
    return (new_mps, log_norm)


def solution(mesh):
    placed = (
        P("col", "sec", None, None, None),
        P("col", None, None, None, None, None),
        P("col", "sec", None, None, None),
        P("col", None, None, None, "sec"),
        P("col", None),
        P("col", None),
        P("col", None),
        P("col", None, None),
    )
    return jax.shard_map(
        local,
        mesh=mesh,
        in_specs=placed,
        out_specs=(P("col", "sec", None, None, None), P()),
        check_vma=False,
    )
```

```python
import functools

import jax
import jax.numpy as jnp
from jax import lax
from jax.experimental import pallas as pl
from jax.experimental.pallas import tpu as pltpu
from jax.sharding import PartitionSpec as P

LANES = 128
PACK = 8
F32 = jnp.float32
BF16 = jnp.bfloat16


def from_behind(x, axis, by):
    count = lax.axis_size(axis)
    return lax.ppermute(x, axis, [(i, (i + by) % count) for i in range(count)])


def chain(
    legs, block, count, cols, secs, left_ref, mps_ref, up_ref, down_ref, right_ref, out_ref, log_ref,
    mps_s, w1, w2, w3, image_s, sq_ref, stage, slots, send_sem, recv_sem,
):
    total = cols * secs
    me_col, me_sec = lax.axis_index("col"), lax.axis_index("sec")
    me = me_col * secs + me_sec
    barrier = pltpu.get_barrier_semaphore()
    step = pl.program_id(0)

    def other(k):
        at = lax.rem(me + k, total)
        return at, (at // secs, lax.rem(at, secs))

    @pl.when(step == 0)
    def _():
        def greet(k, _):
            pl.semaphore_signal(barrier, inc=1, device_id=other(k)[1], device_id_type=pl.DeviceIdType.MESH)
            return 0

        lax.fori_loop(1, total, greet, 0)

    pairs = legs // 2
    rows = legs * PACK
    wide = block * LANES

    @pl.when(pl.program_id(0) == 0)
    def _():
        for uv in range(legs * legs):
            mps_s[:, uv * LANES : (uv + 1) * LANES] = mps_ref[uv]
        sq_ref[...] = jnp.zeros_like(sq_ref)

    for u in range(legs):
        for vp in range(pairs):
            at = (u * legs + 2 * vp) * LANES
            part = jnp.dot(left_ref[...], mps_s[:, at : at + 2 * LANES], preferred_element_type=F32).astype(BF16)
            for x in range(block):
                for mp in range(pairs):
                    lo = x * rows + mp * 2 * PACK
                    for v2 in range(2):
                        w1[vp, mp, v2 * legs + u, :, x * LANES : (x + 1) * LANES] = part[
                            lo : lo + 2 * PACK, v2 * LANES : (v2 + 1) * LANES
                        ]

    slab = w2.shape[2]

    def second(i, _):
        rhs = w1[i // pairs, i % pairs].reshape(2 * legs * 2 * PACK, wide)
        part = jnp.dot(up_ref[...], rhs, preferred_element_type=F32).astype(BF16)
        w2[:, i] = part.reshape(pairs * legs, slab, wide)
        return 0

    lax.fori_loop(0, pairs * pairs, second, 0)

    for dp in range(pairs):
        for r in range(legs):
            rhs = w2[dp * legs + r].reshape(pairs * pairs * slab, wide)
            part = jnp.dot(down_ref[...], rhs, preferred_element_type=F32).astype(BF16)
            for x in range(block):
                for s in range(legs):
                    lane = (r * legs + s) * LANES
                    row = x * rows + dp * 2 * PACK
                    w3[row : row + 2 * PACK, lane : lane + LANES] = part[
                        s * 2 * PACK : (s + 1) * 2 * PACK, x * LANES : (x + 1) * LANES
                    ]

    image = jnp.dot(w3[...], right_ref[...], preferred_element_type=F32)
    here = block * rows
    image_s[pl.ds(pl.multiple_of(step * here, here), here), :] = image
    sq_ref[...] += jnp.sum((image * image).reshape(here // 8, 8, image.shape[1]), axis=0)

    @pl.when(step == pl.num_programs(0) - 1)
    def _():
        mine = jnp.sum(jnp.sum(sq_ref[...], axis=0, keepdims=True), axis=1, keepdims=True)
        stage[...] = jnp.broadcast_to(mine, stage.shape)
        slots[me] = jnp.broadcast_to(mine, stage.shape)
        pl.semaphore_wait(barrier, total - 1)

        def copy_to(k):
            at, where = other(k)
            return pltpu.make_async_remote_copy(
                src_ref=stage,
                dst_ref=slots.at[me],
                send_sem=send_sem.at[k],
                recv_sem=recv_sem.at[me],
                device_id=where,
                device_id_type=pl.DeviceIdType.MESH,
            )

        def send(k, _):
            copy_to(k).start()
            return 0

        def receive(k, _):
            at, where = other(k)
            pltpu.make_async_remote_copy(
                src_ref=stage,
                dst_ref=slots.at[at],
                send_sem=send_sem.at[k],
                recv_sem=recv_sem.at[at],
                device_id=where,
                device_id_type=pl.DeviceIdType.MESH,
            ).wait_recv()
            return 0

        def sent(k, _):
            copy_to(k).wait_send()
            return 0

        lax.fori_loop(1, total, send, 0)
        lax.fori_loop(1, total, receive, 0)
        lax.fori_loop(1, total, sent, 0)
        site = slots[me_col * secs]
        for k in range(1, secs):
            site = site + slots[me_col * secs + k]
        scale = lax.rsqrt(site[0:1, 0:1] / count + 1e-06)
        sums = jnp.sum(slots[...].reshape(cols, secs, 8, LANES), axis=1) / count
        log_ref[...] = jnp.sum(0.5 * jnp.log(sums + 1e-06), axis=0) / cols
        half = image_s.shape[0] // rows
        for d in range(legs):
            for e in range(legs):
                values = image_s[pl.ds(d * PACK + e, half, stride=rows), :]
                out_ref[d * legs + e] = (values * scale).astype(BF16)


def local(mps, ket, left_proj, right_proj, bond_charge, new_charge, link_charge, vert_charge):
    half = left_proj.shape[1]
    full_mps = lax.all_gather(mps, "sec", axis=1, tiled=True)[0]
    chi = full_mps.shape[0]
    legs = full_mps.shape[1]
    phys = ket.shape[5]
    pairs = legs // 2
    rows = legs * PACK
    charges = jnp.concatenate([bond_charge, new_charge, link_charge], axis=1)
    got = from_behind(charges, "col", -1)[0]
    arrived = from_behind(right_proj, "col", -1)
    right = lax.all_gather(arrived, "sec", axis=4, tiled=True)[0]
    q_here = bond_charge[0]
    q_next = got[:chi]
    n_next = got[chi : 2 * chi]
    h_next = got[2 * chi :]
    h_here = link_charge[0]
    n_half = lax.dynamic_slice_in_dim(new_charge[0], lax.axis_index("sec") * half, half, 0)
    upper, lower = vert_charge[0, 0], vert_charge[0, 1]

    keep = (
        q_here[None, None, :, None] + upper[:, None, None, None] - upper[None, :, None, None]
        == q_next[None, None, None, :]
    )
    ms = jnp.where(keep, full_mps.transpose(1, 2, 0, 3), 0).reshape(legs * legs, chi, chi)
    ms = jnp.pad(ms, ((0, 0), (0, 0), (0, LANES - chi)))
    keep = (
        n_half[:, None, None, None]
        == q_here[None, None, None, :] + h_here[None, None, :, None] - h_here[None, :, None, None]
    )
    lp = jnp.where(keep, left_proj[0].transpose(0, 3, 2, 1), 0)
    lp = jnp.pad(lp, ((0, 0), (0, 0), (0, PACK - legs), (0, 0))).reshape(half * rows, chi)
    keep = (
        q_next[None, None, :, None] + h_next[:, None, None, None] - h_next[None, :, None, None]
        == n_next[None, None, None, :]
    )
    rp = jnp.where(keep, right.transpose(1, 2, 0, 3), 0)
    rp = jnp.pad(rp, ((0, 0), (0, 0), (0, LANES - chi), (0, 0))).reshape(legs * legs * LANES, chi)
    physical = jnp.arange(phys, dtype=jnp.int32)
    keep = (
        upper[:, None, None, None, None] + h_here[None, :, None, None, None]
        == lower[None, None, :, None, None] + h_next[None, None, None, :, None] + physical
    )
    ks = jnp.where(keep, ket[0], 0)
    ks8 = jnp.pad(ks, ((0, 0), (0, PACK - legs), (0, 0), (0, 0), (0, 0)))
    two = jnp.eye(2, dtype=BF16)
    up = jnp.einsum(
        "uldcrp,vw,mn->drcvmpwunl", ks8.reshape(legs, PACK, pairs, 2, legs, phys), two, two
    ).reshape(pairs * legs * 8 * phys, 2 * legs * 2 * PACK)
    kd = jnp.pad(ks, ((0, 0), (0, 0), (0, PACK - legs), (0, 0), (0, 0)))
    down = jnp.einsum("vwmnesp,dc->sdevmcwnp", kd.reshape(pairs, 2, pairs, 2, PACK, legs, phys), two).reshape(
        legs * 2 * PACK, pairs * pairs * 8 * phys
    )

    block = 8
    wide = block * LANES
    cols, secs = lax.axis_size("col"), lax.axis_size("sec")
    whole = lambda a: pl.BlockSpec(a.shape, lambda i: (0,) * len(a.shape))
    outs = [
        jax.ShapeDtypeStruct((legs * legs, half, chi), BF16),
        jax.ShapeDtypeStruct((8, LANES), F32),
    ]
    image, logs = pl.pallas_call(
        functools.partial(chain, legs, block, chi * legs * legs * chi, cols, secs),
        grid=(half // block,),
        in_specs=[
            pl.BlockSpec((block * rows, chi), lambda i: (i, 0)),
            whole(ms),
            whole(up),
            whole(down),
            whole(rp),
        ],
        out_specs=[whole(outs[0]), whole(outs[1])],
        out_shape=outs,
        scratch_shapes=[
            pltpu.VMEM((chi, legs * legs * LANES), BF16),
            pltpu.VMEM((pairs, pairs, 2 * legs, 2 * PACK, wide), BF16),
            pltpu.VMEM((pairs * legs, pairs * pairs, 8 * phys, wide), BF16),
            pltpu.VMEM((block * rows, legs * legs * LANES), BF16),
            pltpu.VMEM((half * rows, chi), F32),
            pltpu.VMEM((8, chi), F32),
            pltpu.VMEM((8, LANES), F32),
            pltpu.VMEM((cols * secs, 8, LANES), F32),
            pltpu.SemaphoreType.DMA((cols * secs,)),
            pltpu.SemaphoreType.DMA((cols * secs,)),
        ],
        compiler_params=pltpu.CompilerParams(
            dimension_semantics=("arbitrary",),
            vmem_limit_bytes=56 * 1024 * 1024,
            collective_id=0,
            has_side_effects=True,
        ),
    )(lp, ms, up, down, rp)
    new_mps = image.reshape(legs, legs, half, chi).transpose(2, 0, 1, 3)[None]
    return (new_mps, logs[0, 0])


def solution(mesh):
    placed = (
        P("col", "sec", None, None, None),
        P("col", None, None, None, None, None),
        P("col", "sec", None, None, None),
        P("col", None, None, None, "sec"),
        P("col", None),
        P("col", None),
        P("col", None),
        P("col", None, None),
    )
    return jax.shard_map(
        local,
        mesh=mesh,
        in_specs=placed,
        out_specs=(P("col", "sec", None, None, None), P()),
        check_vma=False,
    )
```

```python
import functools

import jax
import jax.numpy as jnp
import numpy as np
from jax import lax
from jax.experimental import pallas as pl
from jax.experimental.pallas import tpu as pltpu
from jax.sharding import PartitionSpec as P

LANES = 128
PACK = 8
F32 = jnp.float32
BF16 = jnp.bfloat16


MESH = pl.DeviceIdType.MESH


def chain(
    legs, phys, block, count, cols, secs,
    left_ref, mps_ref, right_ref, ket_ref, bond_ref, fresh_ref, link_ref, link_sm, vert_sm,
    index_ref, pick2r, pick2c, same2, pick3r, pick3c, same3,
    out_ref, log_ref,
    left_s, mps_s, right_s, up_ref, down_ref, w1, w2, w3, image_s,
    charge_here, charge_next, mps_all, right_all, diff,
    stage, slots, near_send, near_recv, send_sem, recv_sem,
):
    total = cols * secs
    half, chi = left_ref.shape[1:]
    pairs = legs // 2
    rows = legs * PACK
    wide = block * LANES
    me_col, me_sec = lax.axis_index("col"), lax.axis_index("sec")
    me = me_col * secs + me_sec
    before = lax.rem(me_col + cols - 1, cols)
    barrier = pltpu.get_barrier_semaphore()
    step = pl.program_id(0)
    mine = pl.ds(pl.multiple_of(me_sec * half, 16), half)

    def other(k):
        at = lax.rem(me + k, total)
        return at, (at // secs, lax.rem(at, secs))

    def charge_copy():
        return pltpu.make_async_remote_copy(
            src_ref=charge_here, dst_ref=charge_next, send_sem=near_send.at[0], recv_sem=near_recv.at[0],
            device_id=(before, me_sec), device_id_type=MESH,
        )

    def mps_copy(k, source):
        return pltpu.make_async_remote_copy(
            src_ref=mps_ref, dst_ref=mps_all.at[source], send_sem=near_send.at[k],
            recv_sem=near_recv.at[1 + source],
            device_id=(me_col, lax.rem(me_sec + k, secs)), device_id_type=MESH,
        )

    def right_copy(t, source):
        return pltpu.make_async_remote_copy(
            src_ref=right_ref, dst_ref=right_all.at[source], send_sem=near_send.at[secs + t],
            recv_sem=near_recv.at[1 + secs + source],
            device_id=(before, t), device_id_type=MESH,
        )

    def down_rows(row):
        return jnp.broadcast_to(row, (LANES, LANES)).T

    @pl.when(step == 0)
    def _():
        def greet(k, _):
            pl.semaphore_signal(barrier, inc=1, device_id=other(k)[1], device_id_type=MESH)
            return 0

        lax.fori_loop(1, total, greet, 0)
        charge_here[...] = jnp.zeros_like(charge_here)
        charge_here[0:1, 0:chi] = bond_ref[...]
        charge_here[1:2, 0:chi] = fresh_ref[...]
        charge_here[2:3, 0:legs] = link_ref[...]
        here = charge_here[...].astype(F32)
        diff[...] = down_rows(here[1:2]) - here[0:1]
        left_s[...] = jnp.zeros_like(left_s)
        delta = diff[mine, 0:chi]
        for l in range(legs):
            for m in range(legs):
                gap = (link_sm[0, l] - link_sm[0, m]).astype(F32)
                value = jnp.where(delta == gap, left_ref[l * legs + m].astype(F32), 0.0)
                left_s[pl.ds(m * PACK + l, half, stride=rows), :] = value
        mps_s[...] = jnp.zeros_like(mps_s)
        pl.semaphore_wait(barrier, total - 1)
        charge_copy().start()
        for k in range(1, secs):
            mps_copy(k, me_sec).start()
        for t in range(secs):
            right_copy(t, me_sec).start()
        charge_copy().wait_recv()
        after = charge_next[...].astype(F32)
        diff[...] = after[0:1] - down_rows(here[0:1])

        def place(which, source):
            at = pl.ds(pl.multiple_of(which * half, 16), half)
            delta = diff[at, 0:chi]
            for u in range(legs):
                for v in range(legs):
                    gap = (vert_sm[0, u] - vert_sm[0, v]).astype(F32)
                    uv = u * legs + v
                    value = jnp.where(delta == gap, source[uv].astype(F32), 0.0)
                    mps_s[at, uv * LANES : uv * LANES + chi] = value.astype(BF16)

        place(me_sec, mps_ref)
        lower = index_ref[1].astype(F32)
        upper = jnp.zeros_like(lower)
        for i in range(legs):
            lower += jnp.where(index_ref[0] == i, vert_sm[1, i].astype(F32), 0.0)
            lower += jnp.where(index_ref[2] == i, after[2:3, i : i + 1], 0.0)
            upper += jnp.where(index_ref[3] == i, vert_sm[0, i].astype(F32), 0.0)
            upper += jnp.where(index_ref[4] == i, link_sm[0, i].astype(F32), 0.0)
        ket = jnp.where(upper == lower, ket_ref[...].astype(F32), 0.0).astype(BF16)
        grown = jnp.dot(pick2r[...], ket, preferred_element_type=F32).astype(BF16)
        up_ref[...] = (jnp.dot(grown, pick2c[...], preferred_element_type=F32) * same2[...]).astype(BF16)
        low = jnp.zeros(down_ref.shape, F32)
        for p in range(phys):
            grown = jnp.dot(pick3r[p], ket, preferred_element_type=F32).astype(BF16)
            low += jnp.dot(grown, pick3c[p], preferred_element_type=F32)
        down_ref[...] = (low * same3[...]).astype(BF16)
        for k in range(1, secs):
            source = lax.rem(me_sec + k, secs)
            mps_copy(k, source).wait_recv()
            place(source, mps_all.at[source])

    base = pl.multiple_of(step * (block * rows), block * rows)
    left = left_s[pl.ds(base, block * rows), :].astype(BF16)
    for u in range(legs):
        for vp in range(pairs):
            at = (u * legs + 2 * vp) * LANES
            part = jnp.dot(left, mps_s[:, at : at + 2 * LANES], preferred_element_type=F32).astype(BF16)
            for x in range(block):
                for mp in range(pairs):
                    lo = x * rows + mp * 2 * PACK
                    for v2 in range(2):
                        w1[vp, mp, v2 * legs + u, :, x * LANES : (x + 1) * LANES] = part[
                            lo : lo + 2 * PACK, v2 * LANES : (v2 + 1) * LANES
                        ]

    slab = w2.shape[2]

    def second(i, _):
        rhs = w1[i // pairs, i % pairs].reshape(2 * legs * 2 * PACK, wide)
        part = jnp.dot(up_ref[...], rhs, preferred_element_type=F32).astype(BF16)
        w2[:, i] = part.reshape(pairs * legs, slab, wide)
        return 0

    lax.fori_loop(0, pairs * pairs, second, 0)

    for dp in range(pairs):
        for r in range(legs):
            rhs = w2[dp * legs + r].reshape(pairs * pairs * slab, wide)
            part = jnp.dot(down_ref[...], rhs, preferred_element_type=F32).astype(BF16)
            for x in range(block):
                for s in range(legs):
                    lane = (r * legs + s) * LANES
                    row = pl.multiple_of(base + (x * rows + dp * 2 * PACK), 2 * PACK)
                    w3[pl.ds(row, 2 * PACK), lane : lane + LANES] = part[
                        s * 2 * PACK : (s + 1) * 2 * PACK, x * LANES : (x + 1) * LANES
                    ]

    @pl.when(step == pl.num_programs(0) - 1)
    def _():
        after = charge_next[...].astype(F32)
        diff[...] = down_rows(after[1:2]) - after[0:1]
        right_s[...] = jnp.zeros_like(right_s)
        for k in range(secs):
            right_copy(k, k).wait_recv()
            delta = diff[k * half : (k + 1) * half, 0:chi]
            for r in range(legs):
                for s in range(legs):
                    gap = after[2:3, r : r + 1] - after[2:3, s : s + 1]
                    rs = r * legs + s
                    value = jnp.where(delta == gap, right_all[k, rs].astype(F32), 0.0)
                    right_s[k * half : (k + 1) * half, rs * LANES : rs * LANES + chi] = value.astype(BF16)

        def last(i, square):
            at = pl.ds(pl.multiple_of(i * (block * rows), block * rows), block * rows)
            image = lax.dot_general(
                w3[at, :], right_s[...], (((1,), (1,)), ((), ())), preferred_element_type=F32
            )
            image_s[at, :] = image
            return square + jnp.sum((image * image).reshape(block * rows // 8, 8, chi), axis=0)

        square = lax.fori_loop(0, half // block, last, jnp.zeros((8, chi), F32))
        part = jnp.sum(jnp.sum(square, axis=0, keepdims=True), axis=1, keepdims=True)
        stage[...] = jnp.broadcast_to(part, stage.shape)
        slots[me] = jnp.broadcast_to(part, stage.shape)

        def copy_to(k):
            at, where = other(k)
            return pltpu.make_async_remote_copy(
                src_ref=stage,
                dst_ref=slots.at[me],
                send_sem=send_sem.at[k],
                recv_sem=recv_sem.at[me],
                device_id=where,
                device_id_type=pl.DeviceIdType.MESH,
            )

        def send(k, _):
            copy_to(k).start()
            return 0

        def receive(k, _):
            at, where = other(k)
            pltpu.make_async_remote_copy(
                src_ref=stage,
                dst_ref=slots.at[at],
                send_sem=send_sem.at[k],
                recv_sem=recv_sem.at[at],
                device_id=where,
                device_id_type=pl.DeviceIdType.MESH,
            ).wait_recv()
            return 0

        def sent(k, _):
            copy_to(k).wait_send()
            return 0

        lax.fori_loop(1, total, send, 0)
        lax.fori_loop(1, total, receive, 0)
        lax.fori_loop(1, total, sent, 0)
        charge_copy().wait_send()
        for k in range(1, secs):
            mps_copy(k, me_sec).wait_send()
        for t in range(secs):
            right_copy(t, me_sec).wait_send()
        site = slots[me_col * secs]
        for k in range(1, secs):
            site = site + slots[me_col * secs + k]
        scale = lax.rsqrt(site[0:1, 0:1] / count + 1e-06)
        sums = jnp.sum(slots[...].reshape(cols, secs, 8, LANES), axis=1) / count
        log_ref[...] = jnp.sum(0.5 * jnp.log(sums + 1e-06), axis=0) / cols
        for d in range(legs):
            for e in range(legs):
                values = image_s[pl.ds(d * PACK + e, half, stride=rows), :]
                out_ref[d * legs + e] = (values * scale).astype(BF16)


def picks(legs, phys):
    pairs = legs // 2
    eye = lambda n, m=None: np.eye(n, m, dtype=np.float32)
    d, p, r, u, l = np.meshgrid(*[np.arange(n) for n in (legs, phys, legs, legs, legs)], indexing="ij")
    shape = (legs * phys * legs, legs * legs)
    index = np.stack([d, p, r, u, l]).reshape((5,) + shape).astype(np.int32)
    two = np.ones(2, np.float32)
    dd = eye(legs).reshape(pairs, 2, legs)
    pick2r = np.einsum("icD,rR,v,m,pP->ircvmpDPR", dd, eye(legs), two, two, eye(phys)).reshape(-1, shape[0])
    pick2c = np.einsum("uU,lL,w,n->ulwUnL", eye(legs), eye(legs, PACK), two, two).reshape(shape[1], -1)
    same2 = np.einsum("i,c,p,vw,mn,u,l->icvmpwunl", np.ones(pairs * legs), two, np.ones(phys), eye(2), eye(2),
                      np.ones(legs), np.ones(PACK)).reshape(pick2r.shape[0], -1)
    pick3r = np.einsum("sR,c,De,qP->qsceDPR", eye(legs), two, eye(legs, PACK), eye(phys)).reshape(phys, -1, shape[0])
    pick3c = np.einsum("iav,jbm,c,qp->qvmijcabp", dd, dd, two, eye(phys)).reshape(phys, shape[1], -1)
    same3 = np.einsum("s,dc,e,i,a,p->sdeicap", np.ones(legs), eye(2), np.ones(PACK), np.ones(pairs * pairs),
                      np.ones(4), np.ones(phys)).reshape(pick3r.shape[1], -1)
    out = [jnp.asarray(index)]
    return out + [jnp.asarray(a, BF16) for a in (pick2r, pick2c, same2, pick3r, pick3c, same3)]


def local(mps, ket, left_proj, right_proj, bond_charge, new_charge, link_charge, vert_charge):
    half, chi, legs = left_proj.shape[1:4]
    phys = ket.shape[5]
    pairs = legs // 2
    rows = legs * PACK
    block = 8
    wide = block * LANES
    square = legs * legs
    cols, secs = lax.axis_size("col"), lax.axis_size("sec")
    arrays = [
        left_proj[0].transpose(2, 3, 0, 1).reshape(square, half, chi),
        mps[0].transpose(1, 2, 0, 3).reshape(square, half, chi),
        right_proj[0].transpose(1, 2, 3, 0).reshape(square, half, chi),
        ket[0].transpose(2, 4, 3, 0, 1).reshape(square * phys, square),
        bond_charge,
        new_charge,
        link_charge,
    ]
    small = [link_charge, vert_charge[0]]
    tables = picks(legs, phys)
    whole = lambda a: pl.BlockSpec(a.shape, lambda i: (0,) * len(a.shape))
    scalar = pl.BlockSpec(memory_space=pltpu.SMEM)
    outs = [jax.ShapeDtypeStruct((square, half, chi), BF16), jax.ShapeDtypeStruct((8, LANES), F32)]
    image, logs = pl.pallas_call(
        functools.partial(chain, legs, phys, block, chi * square * chi, cols, secs),
        grid=(half // block,),
        in_specs=[whole(a) for a in arrays] + [scalar] * 2 + [whole(a) for a in tables],
        out_specs=[whole(a) for a in outs],
        out_shape=outs,
        scratch_shapes=[
            pltpu.VMEM((half * rows, chi), F32),
            pltpu.VMEM((chi, square * LANES), BF16),
            pltpu.VMEM((chi, square * LANES), BF16),
            pltpu.VMEM(tables[3].shape, BF16),
            pltpu.VMEM(tables[6].shape, BF16),
            pltpu.VMEM((pairs, pairs, 2 * legs, 2 * PACK, wide), BF16),
            pltpu.VMEM((pairs * legs, pairs * pairs, 8 * phys, wide), BF16),
            pltpu.VMEM((half * rows, square * LANES), BF16),
            pltpu.VMEM((half * rows, chi), F32),
            pltpu.VMEM((8, LANES), jnp.int32),
            pltpu.VMEM((8, LANES), jnp.int32),
            pltpu.VMEM((secs, square, half, chi), BF16),
            pltpu.VMEM((secs, square, half, chi), BF16),
            pltpu.VMEM((LANES, LANES), F32),
            pltpu.VMEM((8, LANES), F32),
            pltpu.VMEM((cols * secs, 8, LANES), F32),
            pltpu.SemaphoreType.DMA((2 * secs,)),
            pltpu.SemaphoreType.DMA((1 + 2 * secs,)),
            pltpu.SemaphoreType.DMA((cols * secs,)),
            pltpu.SemaphoreType.DMA((cols * secs,)),
        ],
        compiler_params=pltpu.CompilerParams(
            dimension_semantics=("arbitrary",),
            vmem_limit_bytes=60 * 1024 * 1024,
            collective_id=0,
            has_side_effects=True,
        ),
    )(*arrays, *small, *tables)
    new_mps = image.reshape(legs, legs, half, chi).transpose(2, 0, 1, 3)[None]
    return (new_mps, logs[0, 0])


def solution(mesh):
    placed = (
        P("col", "sec", None, None, None),
        P("col", None, None, None, None, None),
        P("col", "sec", None, None, None),
        P("col", None, None, None, "sec"),
        P("col", None),
        P("col", None),
        P("col", None),
        P("col", None, None),
    )
    return jax.shard_map(
        local,
        mesh=mesh,
        in_specs=placed,
        out_specs=(P("col", "sec", None, None, None), P()),
        check_vma=False,
    )
```

```python
import functools

import jax
import jax.numpy as jnp
import numpy as np
from jax import lax
from jax.experimental import pallas as pl
from jax.experimental.pallas import tpu as pltpu
from jax.sharding import PartitionSpec as P

LANES = 128
PACK = 8
F32 = jnp.float32
BF16 = jnp.bfloat16


MESH = pl.DeviceIdType.MESH


def chain(
    legs, phys, block, count, cols, secs,
    left_ref, mps_ref, right_ref, ket_ref, bond_ref, fresh_ref, link_ref, link_sm, vert_sm,
    index_ref, pick2r, pick2c, same2, pick3r, pick3c, same3,
    out_ref, log_ref,
    left_s, mps_s, right_s, up_ref, down_ref, w1, w2, w3, image_s,
    charge_here, charge_next, mps_all, right_all, diff,
    stage, slots, near_send, near_recv, send_sem, recv_sem,
):
    total = cols * secs
    half, chi = left_ref.shape[1:]
    pairs = legs // 2
    rows = legs * PACK
    wide = block * LANES
    me_col, me_sec = lax.axis_index("col"), lax.axis_index("sec")
    me = me_col * secs + me_sec
    before = lax.rem(me_col + cols - 1, cols)
    barrier = pltpu.get_barrier_semaphore()
    step = pl.program_id(0)
    mine = pl.ds(pl.multiple_of(me_sec * half, 16), half)

    def other(k):
        at = lax.rem(me + k, total)
        return at, (at // secs, lax.rem(at, secs))

    def close(k):
        at = me_col * secs + lax.rem(me_sec + k, secs)
        return lax.rem(at - me + total, total)

    def charge_copy():
        return pltpu.make_async_remote_copy(
            src_ref=charge_here, dst_ref=charge_next, send_sem=near_send.at[0], recv_sem=near_recv.at[0],
            device_id=(before, me_sec), device_id_type=MESH,
        )

    def mps_copy(k, source):
        return pltpu.make_async_remote_copy(
            src_ref=mps_ref, dst_ref=mps_all.at[source], send_sem=near_send.at[k],
            recv_sem=near_recv.at[1 + source],
            device_id=(me_col, lax.rem(me_sec + k, secs)), device_id_type=MESH,
        )

    def right_copy():
        return pltpu.make_async_remote_copy(
            src_ref=right_ref, dst_ref=right_all.at[me_sec], send_sem=near_send.at[secs],
            recv_sem=near_recv.at[1 + secs + me_sec],
            device_id=(before, me_sec), device_id_type=MESH,
        )

    def right_pass(k, source):
        return pltpu.make_async_remote_copy(
            src_ref=right_all.at[source], dst_ref=right_all.at[source], send_sem=near_send.at[secs + k],
            recv_sem=near_recv.at[1 + secs + source],
            device_id=(me_col, lax.rem(me_sec + k, secs)), device_id_type=MESH,
        )

    def down_rows(row):
        return jnp.broadcast_to(row, (LANES, LANES)).T

    @pl.when(step == 0)
    def _():
        def greet(k, _):
            pl.semaphore_signal(barrier, inc=1, device_id=other(k)[1], device_id_type=MESH)
            return 0

        lax.fori_loop(1, total, greet, 0)
        charge_here[...] = jnp.zeros_like(charge_here)
        charge_here[0:1, 0:chi] = bond_ref[...]
        charge_here[1:2, 0:chi] = fresh_ref[...]
        charge_here[2:3, 0:legs] = link_ref[...]
        here = charge_here[...].astype(F32)
        diff[...] = down_rows(here[1:2]) - here[0:1]
        left_s[...] = jnp.zeros_like(left_s)
        delta = diff[mine, 0:chi]
        for l in range(legs):
            for m in range(legs):
                gap = (link_sm[0, l] - link_sm[0, m]).astype(F32)
                value = jnp.where(delta == gap, left_ref[l * legs + m].astype(F32), 0.0)
                left_s[pl.ds(m * PACK + l, half, stride=rows), :] = value
        mps_s[...] = jnp.zeros_like(mps_s)
        pl.semaphore_wait(barrier, total - 1)
        charge_copy().start()
        for k in range(1, secs):
            mps_copy(k, me_sec).start()
        right_copy().start()
        charge_copy().wait_recv()
        after = charge_next[...].astype(F32)
        diff[...] = after[0:1] - down_rows(here[0:1])

        def place(which, source):
            at = pl.ds(pl.multiple_of(which * half, 16), half)
            delta = diff[at, 0:chi]
            for u in range(legs):
                for v in range(legs):
                    gap = (vert_sm[0, u] - vert_sm[0, v]).astype(F32)
                    uv = u * legs + v
                    value = jnp.where(delta == gap, source[uv].astype(F32), 0.0)
                    mps_s[at, uv * LANES : uv * LANES + chi] = value.astype(BF16)

        place(me_sec, mps_ref)
        lower = index_ref[1].astype(F32)
        upper = jnp.zeros_like(lower)
        for i in range(legs):
            lower += jnp.where(index_ref[0] == i, vert_sm[1, i].astype(F32), 0.0)
            lower += jnp.where(index_ref[2] == i, after[2:3, i : i + 1], 0.0)
            upper += jnp.where(index_ref[3] == i, vert_sm[0, i].astype(F32), 0.0)
            upper += jnp.where(index_ref[4] == i, link_sm[0, i].astype(F32), 0.0)
        ket = jnp.where(upper == lower, ket_ref[...].astype(F32), 0.0).astype(BF16)
        grown = jnp.dot(pick2r[...], ket, preferred_element_type=F32).astype(BF16)
        up_ref[...] = (jnp.dot(grown, pick2c[...], preferred_element_type=F32) * same2[...]).astype(BF16)
        low = jnp.zeros(down_ref.shape, F32)
        for p in range(phys):
            grown = jnp.dot(pick3r[p], ket, preferred_element_type=F32).astype(BF16)
            low += jnp.dot(grown, pick3c[p], preferred_element_type=F32)
        down_ref[...] = (low * same3[...]).astype(BF16)
        for k in range(1, secs):
            source = lax.rem(me_sec + k, secs)
            mps_copy(k, source).wait_recv()
            place(source, mps_all.at[source])

    @pl.when(step == pl.num_programs(0) // 2)
    def _():
        right_copy().wait_recv()
        for k in range(1, secs):
            right_pass(k, me_sec).start()

    base = pl.multiple_of(step * (block * rows), block * rows)
    left = left_s[pl.ds(base, block * rows), :].astype(BF16)
    for u in range(legs):
        for vp in range(pairs):
            at = (u * legs + 2 * vp) * LANES
            part = jnp.dot(left, mps_s[:, at : at + 2 * LANES], preferred_element_type=F32).astype(BF16)
            for x in range(block):
                for mp in range(pairs):
                    lo = x * rows + mp * 2 * PACK
                    for v2 in range(2):
                        w1[vp, mp, v2 * legs + u, :, x * LANES : (x + 1) * LANES] = part[
                            lo : lo + 2 * PACK, v2 * LANES : (v2 + 1) * LANES
                        ]

    slab = w2.shape[2]

    def second(i, _):
        rhs = w1[i // pairs, i % pairs].reshape(2 * legs * 2 * PACK, wide)
        part = jnp.dot(up_ref[...], rhs, preferred_element_type=F32).astype(BF16)
        w2[:, i] = part.reshape(pairs * legs, slab, wide)
        return 0

    lax.fori_loop(0, pairs * pairs, second, 0, unroll=True)

    for dp in range(pairs):
        for r in range(legs):
            rhs = w2[dp * legs + r].reshape(pairs * pairs * slab, wide)
            part = jnp.dot(down_ref[...], rhs, preferred_element_type=F32).astype(BF16)
            for x in range(block):
                for s in range(legs):
                    lane = (r * legs + s) * LANES
                    row = pl.multiple_of(base + (x * rows + dp * 2 * PACK), 2 * PACK)
                    w3[pl.ds(row, 2 * PACK), lane : lane + LANES] = part[
                        s * 2 * PACK : (s + 1) * 2 * PACK, x * LANES : (x + 1) * LANES
                    ]

    @pl.when(step == pl.num_programs(0) - 1)
    def _():
        after = charge_next[...].astype(F32)
        diff[...] = down_rows(after[1:2]) - after[0:1]
        right_s[...] = jnp.zeros_like(right_s)
        for k in range(1, secs):
            right_pass(k, lax.rem(me_sec + k, secs)).wait_recv()
        for k in range(secs):
            delta = diff[k * half : (k + 1) * half, 0:chi]
            for r in range(legs):
                for s in range(legs):
                    gap = after[2:3, r : r + 1] - after[2:3, s : s + 1]
                    rs = r * legs + s
                    value = jnp.where(delta == gap, right_all[k, rs].astype(F32), 0.0)
                    right_s[k * half : (k + 1) * half, rs * LANES : rs * LANES + chi] = value.astype(BF16)

        def last(i, square):
            at = pl.ds(pl.multiple_of(i * (block * rows), block * rows), block * rows)
            image = lax.dot_general(
                w3[at, :], right_s[...], (((1,), (1,)), ((), ())), preferred_element_type=F32
            )
            image_s[at, :] = image
            return square + jnp.sum((image * image).reshape(block * rows // 8, 8, chi), axis=0)

        square = lax.fori_loop(0, half // block, last, jnp.zeros((8, chi), F32))
        part = jnp.sum(jnp.sum(square, axis=0, keepdims=True), axis=1, keepdims=True)
        stage[...] = jnp.broadcast_to(part, stage.shape)
        slots[me] = jnp.broadcast_to(part, stage.shape)

        def copy_to(k):
            at, where = other(k)
            return pltpu.make_async_remote_copy(
                src_ref=stage,
                dst_ref=slots.at[me],
                send_sem=send_sem.at[k],
                recv_sem=recv_sem.at[me],
                device_id=where,
                device_id_type=pl.DeviceIdType.MESH,
            )

        def send(k, _):
            copy_to(k).start()
            return 0

        def receive(k, _):
            at, where = other(k)
            pltpu.make_async_remote_copy(
                src_ref=stage,
                dst_ref=slots.at[at],
                send_sem=send_sem.at[k],
                recv_sem=recv_sem.at[at],
                device_id=where,
                device_id_type=pl.DeviceIdType.MESH,
            ).wait_recv()
            return 0

        def sent(k, _):
            copy_to(k).wait_send()
            return 0

        lax.fori_loop(1, total, send, 0)
        site = jnp.broadcast_to(part, stage.shape)
        for k in range(1, secs):
            receive(close(k), 0)
            site = site + slots[me_col * secs + lax.rem(me_sec + k, secs)]
        scale = lax.rsqrt(site[0:1, 0:1] / count + 1e-06)
        for d in range(legs):
            for e in range(legs):
                values = image_s[pl.ds(d * PACK + e, half, stride=rows), :]
                out_ref[d * legs + e] = (values * scale).astype(BF16)

        def receive_far(k, _):
            at, _where = other(k)

            @pl.when(at // secs != me_col)
            def _():
                receive(k, 0)

            return 0

        lax.fori_loop(1, total, receive_far, 0)
        sums = jnp.sum(slots[...].reshape(cols, secs, 1, LANES), axis=1) / count
        logs = jnp.sum(0.5 * jnp.log(sums + 1e-06), axis=0) / cols
        log_ref[...] = logs[0:1, 0:1]
        lax.fori_loop(1, total, sent, 0)
        charge_copy().wait_send()
        for k in range(1, secs):
            mps_copy(k, me_sec).wait_send()
        right_copy().wait_send()
        for k in range(1, secs):
            right_pass(k, me_sec).wait_send()


def picks(legs, phys):
    pairs = legs // 2
    eye = lambda n, m=None: np.eye(n, m, dtype=np.float32)
    d, p, r, u, l = np.meshgrid(*[np.arange(n) for n in (legs, phys, legs, legs, legs)], indexing="ij")
    shape = (legs * phys * legs, legs * legs)
    index = np.stack([d, p, r, u, l]).reshape((5,) + shape).astype(np.int32)
    two = np.ones(2, np.float32)
    dd = eye(legs).reshape(pairs, 2, legs)
    pick2r = np.einsum("icD,rR,v,m,pP->ircvmpDPR", dd, eye(legs), two, two, eye(phys)).reshape(-1, shape[0])
    pick2c = np.einsum("uU,lL,w,n->ulwUnL", eye(legs), eye(legs, PACK), two, two).reshape(shape[1], -1)
    same2 = np.einsum("i,c,p,vw,mn,u,l->icvmpwunl", np.ones(pairs * legs), two, np.ones(phys), eye(2), eye(2),
                      np.ones(legs), np.ones(PACK)).reshape(pick2r.shape[0], -1)
    pick3r = np.einsum("sR,c,De,qP->qsceDPR", eye(legs), two, eye(legs, PACK), eye(phys)).reshape(phys, -1, shape[0])
    pick3c = np.einsum("iav,jbm,c,qp->qvmijcabp", dd, dd, two, eye(phys)).reshape(phys, shape[1], -1)
    same3 = np.einsum("s,dc,e,i,a,p->sdeicap", np.ones(legs), eye(2), np.ones(PACK), np.ones(pairs * pairs),
                      np.ones(4), np.ones(phys)).reshape(pick3r.shape[1], -1)
    out = [jnp.asarray(index)]
    return out + [jnp.asarray(a, BF16) for a in (pick2r, pick2c, same2, pick3r, pick3c, same3)]


def local(mps, ket, left_proj, right_proj, bond_charge, new_charge, link_charge, vert_charge):
    half, chi, legs = left_proj.shape[1:4]
    phys = ket.shape[5]
    pairs = legs // 2
    rows = legs * PACK
    block = 12
    wide = block * LANES
    square = legs * legs
    cols, secs = lax.axis_size("col"), lax.axis_size("sec")
    arrays = [
        left_proj[0].transpose(2, 3, 0, 1).reshape(square, half, chi),
        mps[0].transpose(1, 2, 0, 3).reshape(square, half, chi),
        right_proj[0].transpose(1, 2, 3, 0).reshape(square, half, chi),
        ket[0].transpose(2, 4, 3, 0, 1).reshape(square * phys, square),
        bond_charge,
        new_charge,
        link_charge,
    ]
    small = [link_charge, vert_charge[0]]
    tables = picks(legs, phys)
    whole = lambda a: pl.BlockSpec(a.shape, lambda i: (0,) * len(a.shape))
    scalar = pl.BlockSpec(memory_space=pltpu.SMEM)
    outs = [jax.ShapeDtypeStruct((square, half, chi), BF16), jax.ShapeDtypeStruct((1, 1), F32)]
    image, logs = pl.pallas_call(
        functools.partial(chain, legs, phys, block, chi * square * chi, cols, secs),
        grid=(half // block,),
        in_specs=[whole(a) for a in arrays] + [scalar] * 2 + [whole(a) for a in tables],
        out_specs=[whole(a) for a in outs],
        out_shape=outs,
        scratch_shapes=[
            pltpu.VMEM((half * rows, chi), F32),
            pltpu.VMEM((chi, square * LANES), BF16),
            pltpu.VMEM((chi, square * LANES), BF16),
            pltpu.VMEM(tables[3].shape, BF16),
            pltpu.VMEM(tables[6].shape, BF16),
            pltpu.VMEM((pairs, pairs, 2 * legs, 2 * PACK, wide), BF16),
            pltpu.VMEM((pairs * legs, pairs * pairs, 8 * phys, wide), BF16),
            pltpu.VMEM((half * rows, square * LANES), BF16),
            pltpu.VMEM((half * rows, chi), F32),
            pltpu.VMEM((8, LANES), jnp.int32),
            pltpu.VMEM((8, LANES), jnp.int32),
            pltpu.VMEM((secs, square, half, chi), BF16),
            pltpu.VMEM((secs, square, half, chi), BF16),
            pltpu.VMEM((LANES, LANES), F32),
            pltpu.VMEM((1, LANES), F32),
            pltpu.VMEM((cols * secs, 1, LANES), F32),
            pltpu.SemaphoreType.DMA((2 * secs,)),
            pltpu.SemaphoreType.DMA((1 + 2 * secs,)),
            pltpu.SemaphoreType.DMA((cols * secs,)),
            pltpu.SemaphoreType.DMA((cols * secs,)),
        ],
        compiler_params=pltpu.CompilerParams(
            dimension_semantics=("arbitrary",),
            vmem_limit_bytes=60 * 1024 * 1024,
            collective_id=0,
            has_side_effects=True,
        ),
    )(*arrays, *small, *tables)
    new_mps = image.reshape(legs, legs, half, chi).transpose(2, 0, 1, 3)[None]
    return (new_mps, logs[0, 0])


def solution(mesh):
    placed = (
        P("col", "sec", None, None, None),
        P("col", None, None, None, None, None),
        P("col", "sec", None, None, None),
        P("col", None, None, None, "sec"),
        P("col", None),
        P("col", None),
        P("col", None),
        P("col", None, None),
    )
    return jax.shard_map(
        local,
        mesh=mesh,
        in_specs=placed,
        out_specs=(P("col", "sec", None, None, None), P()),
        check_vma=False,
    )
```

```python
import functools

import jax
import jax.numpy as jnp
import numpy as np
from jax import lax
from jax.experimental import pallas as pl
from jax.experimental.pallas import tpu as pltpu
from jax.sharding import PartitionSpec as P

LANES = 128
PACK = 8
F32 = jnp.float32
BF16 = jnp.bfloat16


MESH = pl.DeviceIdType.MESH


def chain(
    legs, phys, block, count, cols, secs,
    left_ref, mps_ref, right_ref, ket_ref, bond_ref, fresh_ref, link_ref, link_sm, vert_sm,
    index_ref, pick2r, pick2c, same2, pick3r, pick3c, same3,
    out_ref, log_ref,
    left_s, mps_s, right_s, up_ref, down_ref, w1, w2, w3, image_s,
    charge_here, charge_next, mps_all, right_all, diff,
    stage, slots, near_send, near_recv, send_sem, recv_sem,
):
    total = cols * secs
    half, chi = left_ref.shape[1:]
    pairs = legs // 2
    rows = legs * PACK
    wide = block * LANES
    me_col, me_sec = lax.axis_index("col"), lax.axis_index("sec")
    me = me_col * secs + me_sec
    before = lax.rem(me_col + cols - 1, cols)
    barrier = pltpu.get_barrier_semaphore()
    step = pl.program_id(0)
    mine = pl.ds(pl.multiple_of(me_sec * half, 16), half)

    def other(k):
        at = lax.rem(me + k, total)
        return at, (at // secs, lax.rem(at, secs))

    def close(k):
        at = me_col * secs + lax.rem(me_sec + k, secs)
        return lax.rem(at - me + total, total)

    def charge_copy():
        return pltpu.make_async_remote_copy(
            src_ref=charge_here, dst_ref=charge_next, send_sem=near_send.at[0], recv_sem=near_recv.at[0],
            device_id=(before, me_sec), device_id_type=MESH,
        )

    def mps_copy(k, source):
        return pltpu.make_async_remote_copy(
            src_ref=mps_ref, dst_ref=mps_all.at[source], send_sem=near_send.at[k],
            recv_sem=near_recv.at[1 + source],
            device_id=(me_col, lax.rem(me_sec + k, secs)), device_id_type=MESH,
        )

    def right_copy():
        return pltpu.make_async_remote_copy(
            src_ref=right_ref, dst_ref=right_all.at[me_sec], send_sem=near_send.at[secs],
            recv_sem=near_recv.at[1 + secs + me_sec],
            device_id=(before, me_sec), device_id_type=MESH,
        )

    def right_pass(k, source):
        return pltpu.make_async_remote_copy(
            src_ref=right_all.at[source], dst_ref=right_all.at[source], send_sem=near_send.at[secs + k],
            recv_sem=near_recv.at[1 + secs + source],
            device_id=(me_col, lax.rem(me_sec + k, secs)), device_id_type=MESH,
        )

    def down_rows(row):
        return jnp.broadcast_to(row, (LANES, LANES)).T

    @pl.when(step == 0)
    def _():
        def greet(k, _):
            pl.semaphore_signal(barrier, inc=1, device_id=other(k)[1], device_id_type=MESH)
            return 0

        lax.fori_loop(1, total, greet, 0)
        charge_here[...] = jnp.zeros_like(charge_here)
        charge_here[0:1, 0:chi] = bond_ref[...]
        charge_here[1:2, 0:chi] = fresh_ref[...]
        charge_here[2:3, 0:legs] = link_ref[...]
        here = charge_here[...].astype(F32)
        diff[...] = down_rows(here[1:2]) - here[0:1]
        left_s[...] = jnp.zeros_like(left_s)
        delta = diff[mine, 0:chi]
        for l in range(legs):
            for m in range(legs):
                gap = (link_sm[0, l] - link_sm[0, m]).astype(F32)
                value = jnp.where(delta == gap, left_ref[l * legs + m].astype(F32), 0.0)
                left_s[pl.ds(m * PACK + l, half, stride=rows), :] = value
        mps_s[...] = jnp.zeros_like(mps_s)
        pl.semaphore_wait(barrier, total - 1)
        charge_copy().start()
        for k in range(1, secs):
            mps_copy(k, me_sec).start()
        right_copy().start()
        charge_copy().wait_recv()
        after = charge_next[...].astype(F32)
        diff[...] = after[0:1] - down_rows(here[0:1])

        def place(which, source):
            at = pl.ds(pl.multiple_of(which * half, 16), half)
            delta = diff[at, 0:chi]
            for u in range(legs):
                for v in range(legs):
                    gap = (vert_sm[0, u] - vert_sm[0, v]).astype(F32)
                    uv = u * legs + v
                    value = jnp.where(delta == gap, source[uv].astype(F32), 0.0)
                    mps_s[at, uv * LANES : uv * LANES + chi] = value.astype(BF16)

        place(me_sec, mps_ref)
        lower = index_ref[1].astype(F32)
        upper = jnp.zeros_like(lower)
        for i in range(legs):
            lower += jnp.where(index_ref[0] == i, vert_sm[1, i].astype(F32), 0.0)
            lower += jnp.where(index_ref[2] == i, after[2:3, i : i + 1], 0.0)
            upper += jnp.where(index_ref[3] == i, vert_sm[0, i].astype(F32), 0.0)
            upper += jnp.where(index_ref[4] == i, link_sm[0, i].astype(F32), 0.0)
        ket = jnp.where(upper == lower, ket_ref[...].astype(F32), 0.0).astype(BF16)
        grown = jnp.dot(pick2r[...], ket, preferred_element_type=F32).astype(BF16)
        up_ref[...] = (jnp.dot(grown, pick2c[...], preferred_element_type=F32) * same2[...]).astype(BF16)
        low = jnp.zeros(down_ref.shape, F32)
        for p in range(phys):
            grown = jnp.dot(pick3r[p], ket, preferred_element_type=F32).astype(BF16)
            low += jnp.dot(grown, pick3c[p], preferred_element_type=F32)
        down_ref[...] = (low * same3[...]).astype(BF16)
        for k in range(1, secs):
            source = lax.rem(me_sec + k, secs)
            mps_copy(k, source).wait_recv()
            place(source, mps_all.at[source])

    @pl.when(step == pl.num_programs(0) // 2)
    def _():
        right_copy().wait_recv()
        for k in range(1, secs):
            right_pass(k, me_sec).start()

    base = pl.multiple_of(step * (block * rows), block * rows)
    left = left_s[pl.ds(base, block * rows), :].astype(BF16)
    for u in range(legs):
        for vp in range(pairs):
            at = (u * legs + 2 * vp) * LANES
            part = jnp.dot(left, mps_s[:, at : at + 2 * LANES], preferred_element_type=F32).astype(BF16)
            for x in range(block):
                for mp in range(pairs):
                    lo = x * rows + mp * 2 * PACK
                    for v2 in range(2):
                        w1[vp, mp, v2 * legs + u, :, x * LANES : (x + 1) * LANES] = part[
                            lo : lo + 2 * PACK, v2 * LANES : (v2 + 1) * LANES
                        ]

    slab = w2.shape[2]

    def second(i, _):
        rhs = w1[i // pairs, i % pairs].reshape(2 * legs * 2 * PACK, wide)
        part = jnp.dot(up_ref[...], rhs, preferred_element_type=F32).astype(BF16)
        w2[:, i] = part.reshape(pairs * legs, slab, wide)
        return 0

    lax.fori_loop(0, pairs * pairs, second, 0, unroll=True)

    for dp in range(pairs):
        for r in range(legs):
            rhs = w2[dp * legs + r].reshape(pairs * pairs * slab, wide)
            part = jnp.dot(down_ref[...], rhs, preferred_element_type=F32).astype(BF16)
            for x in range(block):
                for s in range(legs):
                    lane = (r * legs + s) * LANES
                    row = pl.multiple_of(base + (x * rows + dp * 2 * PACK), 2 * PACK)
                    w3[pl.ds(row, 2 * PACK), lane : lane + LANES] = part[
                        s * 2 * PACK : (s + 1) * 2 * PACK, x * LANES : (x + 1) * LANES
                    ]

    @pl.when(step == pl.num_programs(0) - 1)
    def _():
        after = charge_next[...].astype(F32)
        diff[...] = down_rows(after[1:2]) - after[0:1]
        right_s[...] = jnp.zeros_like(right_s)
        for k in range(1, secs):
            right_pass(k, lax.rem(me_sec + k, secs)).wait_recv()
        for k in range(secs):
            delta = diff[k * half : (k + 1) * half, 0:chi]
            for r in range(legs):
                for s in range(legs):
                    gap = after[2:3, r : r + 1] - after[2:3, s : s + 1]
                    rs = r * legs + s
                    value = jnp.where(delta == gap, right_all[k, rs].astype(F32), 0.0)
                    right_s[k * half : (k + 1) * half, rs * LANES : rs * LANES + chi] = value.astype(BF16)

        def last(i, square):
            at = pl.ds(pl.multiple_of(i * (block * rows), block * rows), block * rows)
            image = lax.dot_general(
                w3[at, :], right_s[...], (((1,), (1,)), ((), ())), preferred_element_type=F32
            )
            image_s[at, :] = image
            return square + jnp.sum((image * image).reshape(block * rows // 8, 8, chi), axis=0)

        square = lax.fori_loop(0, half // block, last, jnp.zeros((8, chi), F32), unroll=True)
        part = jnp.sum(jnp.sum(square, axis=0, keepdims=True), axis=1, keepdims=True)
        stage[...] = jnp.broadcast_to(part, stage.shape)
        slots[me] = jnp.broadcast_to(part, stage.shape)

        def copy_to(k):
            at, where = other(k)
            return pltpu.make_async_remote_copy(
                src_ref=stage,
                dst_ref=slots.at[me],
                send_sem=send_sem.at[k],
                recv_sem=recv_sem.at[me],
                device_id=where,
                device_id_type=pl.DeviceIdType.MESH,
            )

        def send(k, _):
            copy_to(k).start()
            return 0

        def receive(k, _):
            at, where = other(k)
            pltpu.make_async_remote_copy(
                src_ref=stage,
                dst_ref=slots.at[at],
                send_sem=send_sem.at[k],
                recv_sem=recv_sem.at[at],
                device_id=where,
                device_id_type=pl.DeviceIdType.MESH,
            ).wait_recv()
            return 0

        def sent(k, _):
            copy_to(k).wait_send()
            return 0

        lax.fori_loop(1, total, send, 0)
        site = jnp.broadcast_to(part, stage.shape)
        for k in range(1, secs):
            receive(close(k), 0)
            site = site + slots[me_col * secs + lax.rem(me_sec + k, secs)]
        scale = lax.rsqrt(site[0:1, 0:1] / count + 1e-06)
        for d in range(legs):
            for e in range(legs):
                values = image_s[pl.ds(d * PACK + e, half, stride=rows), :]
                out_ref[d * legs + e] = (values * scale).astype(BF16)

        def receive_far(k, _):
            at, _where = other(k)

            @pl.when(at // secs != me_col)
            def _():
                receive(k, 0)

            return 0

        lax.fori_loop(1, total, receive_far, 0)
        sums = jnp.sum(slots[...].reshape(cols, secs, 1, LANES), axis=1) / count
        logs = jnp.sum(0.5 * jnp.log(sums + 1e-06), axis=0) / cols
        log_ref[...] = logs[0:1, 0:1]
        lax.fori_loop(1, total, sent, 0)
        charge_copy().wait_send()
        for k in range(1, secs):
            mps_copy(k, me_sec).wait_send()
        right_copy().wait_send()
        for k in range(1, secs):
            right_pass(k, me_sec).wait_send()


def picks(legs, phys):
    pairs = legs // 2
    eye = lambda n, m=None: np.eye(n, m, dtype=np.float32)
    d, p, r, u, l = np.meshgrid(*[np.arange(n) for n in (legs, phys, legs, legs, legs)], indexing="ij")
    shape = (legs * phys * legs, legs * legs)
    index = np.stack([d, p, r, u, l]).reshape((5,) + shape).astype(np.int32)
    two = np.ones(2, np.float32)
    dd = eye(legs).reshape(pairs, 2, legs)
    pick2r = np.einsum("icD,rR,v,m,pP->ircvmpDPR", dd, eye(legs), two, two, eye(phys)).reshape(-1, shape[0])
    pick2c = np.einsum("uU,lL,w,n->ulwUnL", eye(legs), eye(legs, PACK), two, two).reshape(shape[1], -1)
    same2 = np.einsum("i,c,p,vw,mn,u,l->icvmpwunl", np.ones(pairs * legs), two, np.ones(phys), eye(2), eye(2),
                      np.ones(legs), np.ones(PACK)).reshape(pick2r.shape[0], -1)
    pick3r = np.einsum("sR,c,De,qP->qsceDPR", eye(legs), two, eye(legs, PACK), eye(phys)).reshape(phys, -1, shape[0])
    pick3c = np.einsum("iav,jbm,c,qp->qvmijcabp", dd, dd, two, eye(phys)).reshape(phys, shape[1], -1)
    same3 = np.einsum("s,dc,e,i,a,p->sdeicap", np.ones(legs), eye(2), np.ones(PACK), np.ones(pairs * pairs),
                      np.ones(4), np.ones(phys)).reshape(pick3r.shape[1], -1)
    out = [jnp.asarray(index)]
    return out + [jnp.asarray(a, BF16) for a in (pick2r, pick2c, same2, pick3r, pick3c, same3)]


def local(mps, ket, left_proj, right_proj, bond_charge, new_charge, link_charge, vert_charge):
    half, chi, legs = left_proj.shape[1:4]
    phys = ket.shape[5]
    pairs = legs // 2
    rows = legs * PACK
    block = 12
    wide = block * LANES
    square = legs * legs
    cols, secs = lax.axis_size("col"), lax.axis_size("sec")
    arrays = [
        left_proj[0].transpose(2, 3, 0, 1).reshape(square, half, chi),
        mps[0].transpose(1, 2, 0, 3).reshape(square, half, chi),
        right_proj[0].transpose(1, 2, 3, 0).reshape(square, half, chi),
        ket[0].transpose(2, 4, 3, 0, 1).reshape(square * phys, square),
        bond_charge,
        new_charge,
        link_charge,
    ]
    small = [link_charge, vert_charge[0]]
    tables = picks(legs, phys)
    whole = lambda a: pl.BlockSpec(a.shape, lambda i: (0,) * len(a.shape))
    scalar = pl.BlockSpec(memory_space=pltpu.SMEM)
    outs = [jax.ShapeDtypeStruct((square, half, chi), BF16), jax.ShapeDtypeStruct((1, 1), F32)]
    image, logs = pl.pallas_call(
        functools.partial(chain, legs, phys, block, chi * square * chi, cols, secs),
        grid=(half // block,),
        in_specs=[whole(a) for a in arrays] + [scalar] * 2 + [whole(a) for a in tables],
        out_specs=[whole(a) for a in outs],
        out_shape=outs,
        scratch_shapes=[
            pltpu.VMEM((half * rows, chi), F32),
            pltpu.VMEM((chi, square * LANES), BF16),
            pltpu.VMEM((chi, square * LANES), BF16),
            pltpu.VMEM(tables[3].shape, BF16),
            pltpu.VMEM(tables[6].shape, BF16),
            pltpu.VMEM((pairs, pairs, 2 * legs, 2 * PACK, wide), BF16),
            pltpu.VMEM((pairs * legs, pairs * pairs, 8 * phys, wide), BF16),
            pltpu.VMEM((half * rows, square * LANES), BF16),
            pltpu.VMEM((half * rows, chi), F32),
            pltpu.VMEM((8, LANES), jnp.int32),
            pltpu.VMEM((8, LANES), jnp.int32),
            pltpu.VMEM((secs, square, half, chi), BF16),
            pltpu.VMEM((secs, square, half, chi), BF16),
            pltpu.VMEM((LANES, LANES), F32),
            pltpu.VMEM((1, LANES), F32),
            pltpu.VMEM((cols * secs, 1, LANES), F32),
            pltpu.SemaphoreType.DMA((2 * secs,)),
            pltpu.SemaphoreType.DMA((1 + 2 * secs,)),
            pltpu.SemaphoreType.DMA((cols * secs,)),
            pltpu.SemaphoreType.DMA((cols * secs,)),
        ],
        compiler_params=pltpu.CompilerParams(
            dimension_semantics=("arbitrary",),
            vmem_limit_bytes=60 * 1024 * 1024,
            collective_id=0,
            has_side_effects=True,
        ),
    )(*arrays, *small, *tables)
    new_mps = image.reshape(legs, legs, half, chi).transpose(2, 0, 1, 3)[None]
    return (new_mps, logs[0, 0])


def solution(mesh):
    placed = (
        P("col", "sec", None, None, None),
        P("col", None, None, None, None, None),
        P("col", "sec", None, None, None),
        P("col", None, None, None, "sec"),
        P("col", None),
        P("col", None),
        P("col", None),
        P("col", None, None),
    )
    return jax.shard_map(
        local,
        mesh=mesh,
        in_specs=placed,
        out_specs=(P("col", "sec", None, None, None), P()),
        check_vma=False,
    )
```
